32 devices in a mesh: ctx: 4 (over y, x), fsdp: 8 (over z, core).
Axes of the slice: x: 2, y: 2, z: 4, core: 2. Of those that a mesh axis runs over, the one named last changes fastest.
Arguments:
- query_a: bfloat16 [8, 512, 2048], P('fsdp', 'ctx'), may hold values from -64 to 64
- key_a: bfloat16 [8, 512, 256], P('fsdp', 'ctx'), may hold values from -8 to 8
- value_a: bfloat16 [8, 512, 256], P('fsdp', 'ctx'), may hold values from -6 to 6
- resid_in: bfloat16 [8, 512, 1440], P('fsdp', 'ctx'), may hold values from -6 to 6
- doc_lengths: int32 [8, 6], P('fsdp'), may hold values from 1 to 384, 512 in all within a row
- w_out: bfloat16 [2048, 1440], P('fsdp'), may hold values from -0.125 to 0.125
- w_qkv: bfloat16 [1440, 2560], P('fsdp'), may hold values from -8 to 8
- grad_out: bfloat16 [8, 512, 2048], P('fsdp', 'ctx'), may hold values from -6 to 6
- grad_resid: bfloat16 [8, 512, 1440], P('fsdp', 'ctx'), may hold values from -8 to 8
Outputs:
- banded_out: bfloat16 [8, 512, 2048], P('fsdp', 'ctx')
- grad_input: bfloat16 [8, 512, 1440], P('fsdp', 'ctx')
- grad_query: bfloat16 [8, 512, 2048], P('fsdp', 'ctx')
- grad_key: bfloat16 [8, 512, 256], P('fsdp', 'ctx')
- grad_value: bfloat16 [8, 512, 256], P('fsdp', 'ctx')
- grad_w_out: float32 [2048, 1440], P('fsdp')
- grad_w_qkv: float32 [1440, 2560], P('fsdp')
The draws below stay inside these ranges and needn't reach their ends.
Inputs may be any that keep to these rules, and one draw needn't show every extreme that they name: `doc_lengths`: the lengths of a sequence sum to 512, and one document has 384 positions.
All inputs are finite; a program needn't handle non-finite values.
Results may differ from the reference program's by a relative error of at most 0.03.
Values may be sent and summed in bfloat16 or wider, within the bound.
A program may use at most 128 MiB of HBM per device.

```python
import math
import jax
import jax.numpy as jnp
import numpy as np
from jax import lax

H = 32
KV = 4
DH = 64
D = 1440
BAND = 128
DOCS = 6
TOK_DEV = 128
SEQ = 512
SEQS = 8
N_CTX = 4


def drawn_pair(key):
    key_query, key_keys = jax.random.split(key, 2)
    shape_query = (SEQS, SEQ, H * DH)
    shape_keys = (SEQS, SEQ, KV * DH)
    query = jax.random.truncated_normal(key_query, -4.0, 4.0, shape_query, jnp.float32)
    keys = jax.random.truncated_normal(key_keys, -4.0, 4.0, shape_keys, jnp.float32)
    return (query.astype(jnp.bfloat16), keys.astype(jnp.bfloat16))


def draw_query_a(key, part):
    return drawn_pair(jax.random.fold_in(key, 7))[0]


def draw_key_a(key, part):
    return drawn_pair(jax.random.fold_in(key, 7))[1]


def draw_w_qkv(key, part):
    width = (H + 2 * KV) * DH
    matrix = jax.random.truncated_normal(key, -4.0, 4.0, (D, width), jnp.float32) * D ** (-0.5)
    return matrix.astype(jnp.bfloat16)


def draw_grad_resid(key, part):
    key_common, key_rough = jax.random.split(jax.random.fold_in(key, 11))
    common = 0.8 * jax.random.normal(key_common, (SEQS, 1, D), jnp.float32)
    rough = jax.random.normal(key_rough, (SEQS, SEQ, D), jnp.float32)
    return jnp.clip(common + rough, -7.5, 7.5).astype(jnp.bfloat16)


def level_of(key, dims, cuts, low, largest):
    loudness, own = 1.0, jax.random.fold_in(key, 6)
    for position, blocks in cuts:
        draws = jnp.exp(jax.random.uniform(jax.random.fold_in(own, position), (blocks,), jnp.float32, low / len(cuts), largest / len(cuts)))
        loudness = loudness * jnp.repeat(draws, dims[position] // blocks).reshape([-1 if axis == position else 1 for axis in range(len(dims))])
    return loudness


def length_profile(number_of, total, bound, lean):
    loads = [(1 << 20) // math.isqrt(standing ** lean) + 1 for standing in range(2, number_of + 1)]
    surplus, counts = total - bound - (number_of - 1), [1] * (number_of - 1)
    while surplus > 0:
        candidates = [i for i in range(number_of - 1) if counts[i] < bound]
        whole, remaining = sum([loads[i] for i in candidates]), surplus
        for i in candidates:
            extra = min(bound - counts[i], max(1, remaining * loads[i] // whole), surplus)
            counts[i] = counts[i] + extra
            surplus = surplus - extra
    return np.array([bound] + counts)


def ragged(own_key, amount, total, most, skew):
    if amount == 2:
        one = jax.random.randint(own_key, (), max(1, total - most), min(most, total - 1) + 1)
        return jnp.stack([one, total - one])
    sizes = jnp.asarray(length_profile(amount, total, most, skew), jnp.int32)
    twos = (amount - 1) // 2
    source_of, receiver = sizes[1:1 + 2 * twos:2], sizes[2:2 + 2 * twos:2]
    margin = jnp.minimum(source_of - 1, most - receiver)
    shifted = jax.random.randint(jax.random.fold_in(own_key, 1), (twos,), 0, 1 << 20) % (margin + 1)
    sizes = sizes.at[1:1 + 2 * twos:2].set(source_of - shifted).at[2:2 + 2 * twos:2].set(receiver + shifted)
    return sizes[jax.random.permutation(jax.random.fold_in(own_key, 2), amount)]


def normal_values(stream_key, extent, deviation, bound, cuts=(), kind=jnp.bfloat16):
    values = jax.random.normal(stream_key, extent, jnp.float32) * deviation
    if len(cuts) > 0:
        values = level_of(stream_key, extent, cuts, -0.22, 0.18) * values
    return jnp.clip(values, min=-bound, max=bound).astype(kind)


def setup_inputs(seed: int = 0) -> dict:
    key_of = jax.random.split(jax.random.key(seed), 10)
    query_a = draw_query_a(jax.random.fold_in(key_of[9], 71), 0)
    key_a = draw_key_a(jax.random.fold_in(key_of[9], 71), 0)
    value_a = normal_values(key_of[2], (SEQS, SEQ, KV * DH), 1.0, 6.0, ((0, 8), (1, 4)))
    resid_in = normal_values(key_of[3], (SEQS, SEQ, D), 1.0, 6.0, ((0, 8), (1, 4)))
    doc_lengths = jax.vmap(lambda own: ragged(own, DOCS, SEQ, 3 * SEQ // 4, 2))(jax.random.split(key_of[4], SEQS)).reshape((SEQS, DOCS)).astype(jnp.int32)
    w_out = normal_values(key_of[5], (H * DH, D), (H * DH) ** -0.5, 0.125, ((0, 8),))
    w_qkv = draw_w_qkv(jax.random.fold_in(key_of[9], 71), 0)
    grad_out = normal_values(key_of[7], (SEQS, SEQ, H * DH), 1.0, 6.0, ((0, 8), (1, 4)))
    grad_resid = draw_grad_resid(jax.random.fold_in(key_of[9], 71), 0)
    return dict(query_a=query_a, key_a=key_a, value_a=value_a, resid_in=resid_in, doc_lengths=doc_lengths, w_out=w_out, w_qkv=w_qkv, grad_out=grad_out, grad_resid=grad_resid)


MASKED = -1e+30
EPSILON = 1e-05

def doc_index(lengths):
    ends = jnp.cumsum(lengths)
    places = jnp.arange(SEQ, dtype=jnp.int32)
    return lax.optimization_barrier(jnp.sum((places[:, None] >= ends[None, :]).astype(jnp.int32), axis=1))

def allowed_pairs(documents, reach):
    places = jnp.arange(SEQ, dtype=jnp.int32)
    behind = places[:, None] - places[None, :]
    same_doc = documents[:, None] == documents[None, :]
    return same_doc & (behind >= 0) & (behind < reach)

def query_heads(rows):
    return rows.reshape(SEQ, KV, H // KV, DH).transpose(1, 2, 0, 3)

def pair_heads(rows):
    return rows.reshape(SEQ, KV, DH).transpose(1, 0, 2)

def merge_query(heads):
    return heads.transpose(2, 0, 1, 3).reshape(SEQ, H * DH)

def merge_pair(heads):
    return heads.transpose(1, 0, 2).reshape(SEQ, KV * DH)

def attention_weights(query_group, key_head, allowed):
    scores = jnp.einsum('gid,jd->gij', query_group.astype(jnp.float32), key_head.astype(jnp.float32)) * DH ** (-0.5)
    scores = jnp.where(allowed, scores, MASKED)
    row_max = lax.optimization_barrier(jnp.max(scores, axis=-1, keepdims=True))
    log_total = row_max + jnp.log(lax.optimization_barrier(jnp.sum(jnp.where(allowed, jnp.exp(scores - row_max), 0.0), axis=-1, keepdims=True)))
    return jnp.where(allowed, jnp.exp(scores - log_total), 0.0)

def attend(query, keys, values, allowed):

    def one_head(items):
        query_group, key_head, value_head = items
        weights = attention_weights(query_group, key_head, allowed).astype(jnp.bfloat16)
        summed = jnp.einsum('gij,jd->gid', weights.astype(jnp.float32), value_head.astype(jnp.float32))
        return summed.astype(jnp.bfloat16)
    return merge_query(lax.map(one_head, (query_heads(query), pair_heads(keys), pair_heads(values))))

def attend_back(query, keys, values, output, grad, allowed):

    def one_head(items):
        query_group, key_head, value_head, out_group, grad_group = items
        weights = attention_weights(query_group, key_head, allowed)
        weights_bf = weights.astype(jnp.bfloat16)
        grad_weights = jnp.einsum('gid,jd->gij', grad_group.astype(jnp.float32), value_head.astype(jnp.float32))
        correction = lax.optimization_barrier(jnp.sum(grad_group.astype(jnp.float32) * out_group.astype(jnp.float32), axis=-1, keepdims=True))
        grad_scores = (weights * (grad_weights - correction)).astype(jnp.bfloat16)
        grad_q = jnp.einsum('gij,jd->gid', grad_scores.astype(jnp.float32), key_head.astype(jnp.float32)) * DH ** (-0.5)
        grad_k = jnp.einsum('gij,gid->jd', grad_scores.astype(jnp.float32), query_group.astype(jnp.float32)) * DH ** (-0.5)
        grad_v = jnp.einsum('gij,gid->jd', weights_bf.astype(jnp.float32), grad_group.astype(jnp.float32))
        return (grad_q.astype(jnp.bfloat16), grad_k.astype(jnp.bfloat16), grad_v.astype(jnp.bfloat16))
    items = (query_heads(query), pair_heads(keys), pair_heads(values), query_heads(output), query_heads(grad))
    grad_q, grad_k, grad_v = lax.map(one_head, items)
    return (merge_query(grad_q), merge_pair(grad_k), merge_pair(grad_v))

def block_terms(left, right, total):
    left_blocks = left.reshape(N_CTX, TOK_DEV, left.shape[1])
    right_blocks = right.reshape(N_CTX, TOK_DEV, right.shape[1])

    def add_block(acc, pieces):
        left_piece, right_piece = pieces
        term = jnp.dot(left_piece.T, right_piece, preferred_element_type=jnp.float32).astype(jnp.bfloat16)
        term = lax.optimization_barrier(term)
        return (acc + term.astype(jnp.float32), None)
    total, unused = lax.scan(add_block, total, (left_blocks, right_blocks))
    return total

def reference(query_a, key_a, value_a, resid_in, doc_lengths, w_out, w_qkv, grad_out, grad_resid):

    def one_sequence(carry, items):
        sum_out, sum_qkv = carry
        query, keys, values, resid, lengths, grad_o, grad_r = items
        documents = doc_index(lengths)
        full_allowed = allowed_pairs(documents, SEQ)
        band_allowed = allowed_pairs(documents, BAND)
        attended = attend(query, keys, values, full_allowed)
        resid_mid = (resid.astype(jnp.float32) + jnp.dot(attended, w_out, preferred_element_type=jnp.float32)).astype(jnp.bfloat16)
        resid_f = resid_mid.astype(jnp.float32)
        inverse_rms = lax.rsqrt(lax.optimization_barrier(jnp.mean(resid_f * resid_f, axis=-1, keepdims=True)) + EPSILON)
        normed = resid_f * inverse_rms
        normed_bf = normed.astype(jnp.bfloat16)
        projected = jnp.dot(normed_bf, w_qkv, preferred_element_type=jnp.float32).astype(jnp.bfloat16)
        query_b = projected[:, :H * DH]
        key_b = projected[:, H * DH:H * DH + KV * DH]
        value_b = projected[:, H * DH + KV * DH:]
        banded = attend(query_b, key_b, value_b, band_allowed)
        grad_qb, grad_kb, grad_vb = attend_back(query_b, key_b, value_b, banded, grad_o, band_allowed)
        grad_proj = jnp.concatenate([grad_qb, grad_kb, grad_vb], axis=1)
        grad_normed = jnp.dot(grad_proj, w_qkv.T, preferred_element_type=jnp.float32)
        middle = lax.optimization_barrier(jnp.mean(grad_normed * normed, axis=-1, keepdims=True))
        grad_mid = (grad_r.astype(jnp.float32) + inverse_rms * (grad_normed - normed * middle)).astype(jnp.bfloat16)
        grad_attended = jnp.dot(grad_mid, w_out.T, preferred_element_type=jnp.float32).astype(jnp.bfloat16)
        grad_q, grad_k, grad_v = attend_back(query, keys, values, attended, grad_attended, full_allowed)
        sum_out = block_terms(attended, grad_mid, sum_out)
        sum_qkv = block_terms(normed_bf, grad_proj, sum_qkv)
        return ((sum_out, sum_qkv), (banded, grad_mid, grad_q, grad_k, grad_v))
    items = (query_a, key_a, value_a, resid_in, doc_lengths, grad_out, grad_resid)
    start = (jnp.zeros(w_out.shape, jnp.float32), jnp.zeros(w_qkv.shape, jnp.float32))
    (grad_w_out, grad_w_qkv), outputs = lax.scan(one_sequence, start, items)
    banded_out, grad_input, grad_query, grad_key, grad_value = outputs
    return (banded_out, grad_input, grad_query, grad_key, grad_value, grad_w_out, grad_w_qkv)
```

```python
import functools

import jax
import jax.numpy as jnp
from jax import lax
from jax.experimental import pallas as pl
from jax.experimental.pallas import tpu as pltpu
from jax.sharding import PartitionSpec as P

H = 32
KV = 4
DH = 64
BAND = 128


MASKED = -1e30
EPSILON = 1e-05


def from_behind(value, axis, steps):
    count = lax.axis_size(axis)
    leading, last = (max(0, -steps), min(count, count - steps))
    return lax.ppermute(value, axis, [(source, source + steps) for source in range(leading, last)])


def doc_table(lengths, seq_len):
    ends = jnp.cumsum(lengths)
    places = jnp.arange(seq_len, dtype=jnp.int32)
    before = places[:, None] >= ends[None, :]
    return jnp.sum(before.astype(jnp.int32), axis=1)


def attend_kernel(with_output, with_grads, *refs):
    refs = list(refs)
    allowed_ref, q_ref, k_ref, v_ref, v_t_ref = refs[:5]
    del refs[:5]
    if with_grads:
        k_t_ref, g_ref = refs[:2]
        del refs[:2]
    o_ref = refs.pop(0)
    if with_grads:
        dq_ref, dk_ref, dv_ref = refs
    allowed = allowed_ref[...] > 0.0
    keys, values, values_t = (k_ref[0], v_ref[0], v_t_ref[...])
    dk = jnp.zeros(keys.shape, jnp.float32)
    dv = jnp.zeros(keys.shape, jnp.float32)
    by_last = (((1,), (1,)), ((), ()))
    for head in range(H // KV):
        rows = slice(head * DH, (head + 1) * DH)
        query = q_ref[rows, :]
        scores = jnp.dot(keys, query, preferred_element_type=jnp.float32) * DH ** (-0.5)
        scores = jnp.where(allowed, scores, MASKED)
        row_max = jnp.max(scores, axis=0, keepdims=True)
        log_total = row_max + jnp.log(
            jnp.sum(jnp.exp(scores - row_max), axis=0, keepdims=True)
        )
        weights = jnp.where(allowed, jnp.exp(scores - log_total), 0.0)
        weights_bf = weights.astype(jnp.bfloat16)
        if with_output:
            output = jnp.dot(values_t, weights_bf, preferred_element_type=jnp.float32)
            output = output.astype(jnp.bfloat16)
            o_ref[rows, :] = output
        else:
            output = o_ref[rows, :]
        if with_grads:
            grad = g_ref[rows, :]
            correction = jnp.sum(
                grad.astype(jnp.float32) * output.astype(jnp.float32), axis=0, keepdims=True
            )
            grad_weights = jnp.dot(values, grad, preferred_element_type=jnp.float32)
            grad_scores = (weights * (grad_weights - correction)).astype(jnp.bfloat16)
            grad_q = jnp.dot(k_t_ref[...], grad_scores, preferred_element_type=jnp.float32)
            dq_ref[rows, :] = (grad_q * DH ** (-0.5)).astype(jnp.bfloat16)
            dk += lax.dot_general(grad_scores, query, by_last, preferred_element_type=jnp.float32)
            dv += lax.dot_general(weights_bf, grad, by_last, preferred_element_type=jnp.float32)
    if with_grads:
        dk_ref[0] = dk
        dv_ref[0] = dv


def by_head(rows):
    return rows.reshape(rows.shape[0], KV, DH).transpose(1, 0, 2)


def from_heads(heads):
    return heads.transpose(1, 0, 2).reshape(heads.shape[1], KV * DH)


def attend(allowed_t, query_t, keys, values, output_t=None, grad_t=None):
    columns, rows = allowed_t.shape
    with_output, with_grads = (output_t is None, grad_t is not None)
    group = pl.BlockSpec((query_t.shape[0] // KV, rows), lambda g: (g, 0))
    key_rows = pl.BlockSpec((1, columns, DH), lambda g: (g, 0, 0))
    key_columns = pl.BlockSpec((DH, columns), lambda g: (g, 0))
    args = [allowed_t, query_t, by_head(keys), by_head(values), values.T]
    in_specs = [pl.BlockSpec((columns, rows), lambda g: (0, 0)), group]
    in_specs += [key_rows, key_rows, key_columns]
    out_shape, out_specs = ([], [])
    wide = jax.ShapeDtypeStruct(query_t.shape, jnp.bfloat16)
    narrow = jax.ShapeDtypeStruct((KV, columns, DH), jnp.float32)
    if with_grads:
        args += [keys.T, grad_t]
        in_specs += [key_columns, group]
    if with_output:
        out_shape.append(wide)
        out_specs.append(group)
    else:
        args.append(output_t)
        in_specs.append(group)
    if with_grads:
        out_shape += [wide, narrow, narrow]
        out_specs += [group, key_rows, key_rows]
    return pl.pallas_call(
        functools.partial(attend_kernel, with_output, with_grads),
        grid=(KV,),
        out_shape=tuple(out_shape),
        in_specs=in_specs,
        out_specs=tuple(out_specs),
    )(*args)


MESH = pl.DeviceIdType.MESH


def remote(src, dst, send_sem, recv_sem, ctx, fsdp):
    return pltpu.make_async_remote_copy(
        src_ref=src,
        dst_ref=dst,
        send_sem=send_sem,
        recv_sem=recv_sem,
        device_id={"ctx": ctx, "fsdp": fsdp},
        device_id_type=MESH,
    )


def place():
    return (lax.axis_index("ctx"), lax.axis_index("fsdp"))


def shard_at(z, core, planes, offset):
    return 2 * lax.rem(z + offset, planes) + core


def greet(planes):
    c, f = place()
    z, core = (f // 2, lax.rem(f, 2))
    barrier = pltpu.get_barrier_semaphore()
    peers = [(c ^ 1, f), (c ^ 2, f), (c ^ 3, f), (c, f ^ 1)]
    peers += [(c, shard_at(z, core, planes, d)) for d in range(1, planes)]
    for ctx, fsdp in peers:
        pl.semaphore_signal(
            barrier, inc=1, device_id={"ctx": ctx, "fsdp": fsdp}, device_id_type=MESH
        )
    pl.semaphore_wait(barrier, len(peers))


def quarter_of(ref, weight, quarter):
    if weight == 0:
        size = ref.shape[0] // 4
        return ref.at[pl.ds(pl.multiple_of(quarter * size, 16), size), :]
    size = ref.shape[1] // 4
    return ref.at[:, pl.ds(pl.multiple_of(quarter * size, 128), size)]


def by_distance(planes):
    order = []
    for step in range(1, planes // 2 + 1):
        for d in (step, planes - step):
            if d not in order:
                order.append(d)
    return order


def gather_kernel(
    planes, wo, wq, kv, go, gq, gkv, send, recv_z, recv_x, recv_y, recv_d, recv_p, recv_kv, local
):
    c, f = place()
    z, core = (f // 2, lax.rem(f, 2))
    mine, full = ((wo, wq), (go, gq))
    rows = kv.shape[0]
    owns = [
        pltpu.make_async_copy(kv, gkv.at[pl.ds(pl.multiple_of(c * rows, 128), rows)], local),
        pltpu.make_async_copy(wo, go.at[f], local),
        pltpu.make_async_copy(wq, gq.at[f], local),
    ]
    for copy in owns:
        copy.start()
    greet(planes)
    started = []

    def push(*args):
        copy = remote(*args)
        copy.start()
        started.append(copy)

    def piece(weight, shard, quarter):
        return quarter_of(full[weight].at[shard], weight, quarter)

    def arrive(ref, sem):
        remote(ref, ref, send, sem, c ^ 1, f).wait_recv()

    kv_place = gkv.at[pl.ds(pl.multiple_of(c * rows, 128), rows)]
    for i, bit in enumerate((1, 2, 3)):
        push(kv, kv_place, send, recv_kv.at[i], c ^ bit, f)
    order = by_distance(planes)
    for weight in (0, 1):
        for d in order:
            push(
                quarter_of(mine[weight], weight, c),
                piece(weight, f, c),
                send,
                recv_z.at[weight, d],
                c,
                shard_at(z, core, planes, d),
            )
        push(mine[weight], full[weight].at[f], send, recv_p.at[weight, 0, 0], c, f ^ 1)
    steps = [(weight, d) for weight in (0, 1) for d in order]

    def to_partner(weight, d, shard, slot):
        part = piece(weight, shard, c ^ slot)
        push(part, part, send, recv_p.at[weight, d, slot], c, f ^ 1)

    def first(weight, d):
        shard = shard_at(z, core, planes, planes - d)
        part = piece(weight, shard, c)
        arrive(part, recv_z.at[weight, d])
        push(part, part, send, recv_x.at[weight, d], c ^ 1, f)
        push(part, part, send, recv_y.at[weight, d], c ^ 2, f)
        to_partner(weight, d, shard, 0)

    def second(weight, d):
        shard = shard_at(z, core, planes, planes - d)
        arrive(piece(weight, shard, c ^ 1), recv_x.at[weight, d])
        arrive(piece(weight, shard, c ^ 2), recv_y.at[weight, d])
        bit = jnp.where(core == weight, 1, 2)
        part = piece(weight, shard, c ^ bit)
        push(part, part, send, recv_d.at[weight, d], c ^ (3 - bit), f)
        to_partner(weight, d, shard, 1)
        to_partner(weight, d, shard, 2)

    def third(weight, d):
        shard = shard_at(z, core, planes, planes - d)
        arrive(piece(weight, shard, c ^ 3), recv_d.at[weight, d])
        to_partner(weight, d, shard, 3)

    count = len(steps)
    for i in range(count + 2):
        if i < count:
            first(*steps[i])
        if 0 <= i - 1 < count:
            second(*steps[i - 1])
        if 0 <= i - 2 < count:
            third(*steps[i - 2])
    for weight in (0, 1):
        arrive(full[weight].at[f ^ 1], recv_p.at[weight, 0, 0])
        for d in order:
            shard = shard_at(z, core, planes, planes - d) ^ 1
            for slot in range(4):
                arrive(piece(weight, shard, c ^ slot), recv_p.at[weight, d, slot])
    for i in range(3):
        arrive(kv_place, recv_kv.at[i])
    for copy in started:
        copy.wait_send()
    for copy in owns:
        copy.wait()


def gather_weights(w_out, w_qkv, kv):
    count = lax.axis_size("fsdp")
    planes = count // 2
    dma = pltpu.SemaphoreType.DMA
    anywhere = pl.BlockSpec(memory_space=pl.ANY)
    return pl.pallas_call(
        functools.partial(gather_kernel, planes),
        out_shape=(
            jax.ShapeDtypeStruct((count,) + w_out.shape, w_out.dtype),
            jax.ShapeDtypeStruct((count,) + w_qkv.shape, w_qkv.dtype),
            jax.ShapeDtypeStruct((4 * kv.shape[0], kv.shape[1]), kv.dtype),
        ),
        in_specs=[anywhere] * 3,
        out_specs=(anywhere,) * 3,
        scratch_shapes=[
            dma,
            dma((2, planes)),
            dma((2, planes)),
            dma((2, planes)),
            dma((2, planes)),
            dma((2, planes, 4)),
            dma((3,)),
            dma,
        ],
        compiler_params=pltpu.CompilerParams(collective_id=0, has_side_effects=True),
    )(w_out, w_qkv, kv)


def reduce_kernel(
    planes,
    att_t,
    norm_t,
    grad_mid,
    grad_proj,
    kv_sums,
    out_o,
    out_q,
    out_kv,
    a_o,
    a_q,
    s_o,
    s_q,
    p_o,
    p_q,
    r1_o,
    r1_q,
    r2_o,
    r2_q,
    rz_o,
    rz_q,
    from_kv,
    send,
    recv_p,
    recv_1,
    recv_2,
    recv_z,
    recv_f,
    recv_kv,
):
    c, f = place()
    z, core = (f // 2, lax.rem(f, 2))
    greet(planes)
    own, sent, from_p, from_1, from_2, from_z, result = (
        (a_o, a_q),
        (s_o, s_q),
        (p_o, p_q),
        (r1_o, r1_q),
        (r2_o, r2_q),
        (rz_o, rz_q),
        (out_o, out_q),
    )
    started = []

    def push(*args):
        copy = remote(*args)
        copy.start()
        started.append(copy)

    def arrive(ref, sem):
        remote(ref, ref, send, sem, c ^ 1, f).wait_recv()

    def term(weight, shard):
        if weight == 0:
            size = a_o.shape[1]
            left = att_t[pl.ds(pl.multiple_of(shard * size, size), size), :]
            right = grad_mid[...]
        else:
            left = norm_t[shard]
            right = grad_proj[...]
        return jnp.dot(left, right, preferred_element_type=jnp.float32).astype(jnp.bfloat16)

    def added(first, second):
        return (first.astype(jnp.float32) + second.astype(jnp.float32)).astype(jnp.bfloat16)

    rows = out_kv.shape[0]

    def kv_rows(index):
        return kv_sums.at[pl.ds(pl.multiple_of(index * rows, rows), rows), :]

    for slot in (3, 1, 2):
        push(
            kv_rows(c ^ slot), from_kv.at[slot], send, recv_kv.at[slot], c ^ slot, f
        )
    order = by_distance(planes)[::-1] + [0]
    steps = [(weight, d) for d in order for weight in (1, 0)]

    def bits(weight):
        bit = jnp.where(core == weight, 1, 2)
        return (bit, 3 - bit)

    def produce(weight, d):
        shard = shard_at(z, core, planes, d)
        sent[weight][d] = term(weight, shard ^ 1)
        push(sent[weight].at[d], from_p[weight].at[d], send, recv_p.at[weight, d], c, f ^ 1)
        own[weight][d] = term(weight, shard)

    def chip_sum(weight, d):
        arrive(from_p[weight].at[d], recv_p.at[weight, d])
        own[weight][d] = added(own[weight][d], from_p[weight][d])
        bit, other = bits(weight)
        for slot, quarter in ((1, c ^ 3), (0, c ^ bit)):
            push(
                quarter_of(own[weight].at[d], weight, quarter),
                from_1[weight].at[d, slot],
                send,
                recv_1.at[weight, d, slot],
                c ^ bit,
                f,
            )

    def pair_sum(weight, d):
        bit, other = bits(weight)
        for slot, quarter in ((1, c ^ other), (0, c)):
            arrive(from_1[weight].at[d, slot], recv_1.at[weight, d, slot])
            part = quarter_of(own[weight].at[d], weight, quarter)
            part[...] = added(part[...], from_1[weight][d, slot])
            if slot == 1:
                push(part, from_2[weight].at[d], send, recv_2.at[weight, d], c ^ other, f)

    def plane_sum(weight, d):
        arrive(from_2[weight].at[d], recv_2.at[weight, d])
        part = quarter_of(own[weight].at[d], weight, c)
        part[...] = added(part[...], from_2[weight][d])
        if d:
            push(
                part,
                from_z[weight].at[d],
                send,
                recv_z.at[weight, d],
                c,
                shard_at(z, core, planes, d),
            )

    def finish(weight):
        part = quarter_of(own[weight].at[0], weight, c)
        total = part[...].astype(jnp.float32)
        for d in range(1, planes):
            arrive(from_z[weight].at[d], recv_z.at[weight, d])
            total = total + from_z[weight][d].astype(jnp.float32)
        place_c = quarter_of(result[weight], weight, c)
        place_c[...] = total.astype(jnp.bfloat16)
        for slot in (3, 1, 2):
            push(place_c, place_c, send, recv_f.at[weight, slot], c ^ slot, f)

    stages = (produce, chip_sum, pair_sum, plane_sum)
    lags = (0, 2, 4, 6)
    count = len(steps)
    for i in range(count + lags[-1]):
        for stage, lag in zip(stages, lags):
            if 0 <= i - lag < count:
                stage(*steps[i - lag])
    kv_total = kv_rows(c)[...].astype(jnp.float32)
    for slot in (1, 2, 3):
        arrive(from_kv.at[slot], recv_kv.at[slot])
        kv_total += from_kv[slot].astype(jnp.float32)
    out_kv[...] = kv_total
    for weight in (1, 0):
        finish(weight)
    for weight in (1, 0):
        for slot in (3, 1, 2):
            arrive(quarter_of(result[weight], weight, c ^ slot), recv_f.at[weight, slot])
    for copy in started:
        copy.wait_send()


def reduce_weights(att_t, norm_t, grad_mid, grad_proj, kv_sums):
    count = lax.axis_size("fsdp")
    planes = count // 2
    dma = pltpu.SemaphoreType.DMA
    in_vmem = pl.BlockSpec(memory_space=pltpu.VMEM)
    bf = jnp.bfloat16
    o_shape = (att_t.shape[0] // count, grad_mid.shape[1])
    q_shape = (norm_t.shape[1], grad_proj.shape[1])
    o_part = (o_shape[0] // 4, o_shape[1])
    q_part = (q_shape[0], q_shape[1] // 4)
    scratch = []
    for lead, shapes in (
        ((planes,), (o_shape, q_shape)),
        ((planes,), (o_shape, q_shape)),
        ((planes,), (o_shape, q_shape)),
        ((planes, 2), (o_part, q_part)),
        ((planes,), (o_part, q_part)),
        ((planes,), (o_part, q_part)),
    ):
        scratch += [pltpu.VMEM(lead + shape, bf) for shape in shapes]
    kv_shape = (kv_sums.shape[0] // 4, kv_sums.shape[1])
    scratch.append(pltpu.VMEM((4,) + kv_shape, bf))
    return pl.pallas_call(
        functools.partial(reduce_kernel, planes),
        out_shape=(
            jax.ShapeDtypeStruct(o_shape, bf),
            jax.ShapeDtypeStruct(q_shape, bf),
            jax.ShapeDtypeStruct(kv_shape, jnp.float32),
        ),
        in_specs=[in_vmem] * 5,
        out_specs=(in_vmem,) * 3,
        scratch_shapes=scratch
        + [
            dma,
            dma((2, planes)),
            dma((2, planes, 2)),
            dma((2, planes)),
            dma((2, planes)),
            dma((2, 4)),
            dma((4,)),
        ],
        compiler_params=pltpu.CompilerParams(
            collective_id=1, has_side_effects=True, vmem_limit_bytes=60 * 2**20
        ),
    )(att_t, norm_t, grad_mid, grad_proj, kv_sums)


def per_device(query_a, key_a, value_a, resid_in, doc_lengths, w_out, w_qkv, grad_out, grad_resid):
    ctx_count = lax.axis_size("ctx")
    ctx_index = lax.axis_index("ctx")
    local_rows = query_a.shape[1]
    seq_len = local_rows * ctx_count
    band_len = BAND
    first_row = ctx_index * local_rows
    documents = doc_table(doc_lengths[0], seq_len)
    fsdp_count = lax.axis_size("fsdp")
    own_kernels = ctx_count == 4 and fsdp_count % 2 == 0 and w_out.shape[0] % 64 == 0
    if own_kernels:
        w_o3, w_b3, kv = gather_weights(
            w_out, w_qkv, jnp.concatenate([key_a[0], value_a[0]], axis=1)
        )
        w_o = w_o3.reshape(-1, w_out.shape[1])
        w_b = w_b3.reshape(-1, w_qkv.shape[1])
        keys, values = (kv[:, : KV * DH], kv[:, KV * DH :])
    else:
        w_o, w_b = (
            lax.all_gather(w_out, "fsdp", axis=0, tiled=True),
            lax.all_gather(w_qkv, "fsdp", axis=0, tiled=True),
        )
        keys, values = (
            lax.all_gather(key_a[0], "ctx", axis=0, tiled=True),
            lax.all_gather(value_a[0], "ctx", axis=0, tiled=True),
        )
    query_t = query_a[0].T
    row_docs = lax.dynamic_slice_in_dim(documents, first_row, local_rows)[None, :]
    row_places = (first_row + jnp.arange(local_rows, dtype=jnp.int32))[None, :]
    columns = jnp.arange(seq_len, dtype=jnp.int32)[:, None]
    allowed_t = ((documents[:, None] == row_docs) & (columns <= row_places)).astype(jnp.float32)
    (attended_t,) = attend(allowed_t, query_t, keys, values)
    attended = attended_t.T
    resid_mid = (
        resid_in[0].astype(jnp.float32) + jnp.dot(attended, w_o, preferred_element_type=jnp.float32)
    ).astype(jnp.bfloat16)
    resid_f = resid_mid.astype(jnp.float32)
    inverse_rms = lax.rsqrt(jnp.mean(resid_f * resid_f, axis=-1, keepdims=True) + EPSILON)
    normed = resid_f * inverse_rms
    normed_bf = normed.astype(jnp.bfloat16)
    projected = jnp.dot(normed_bf, w_b, preferred_element_type=jnp.float32).astype(jnp.bfloat16)
    query_b = projected[:, : H * DH]
    key_b = projected[:, H * DH : H * DH + KV * DH]
    value_b = projected[:, H * DH + KV * DH :]
    tails = from_behind(projected[:, H * DH :], "ctx", 1)
    tail_keys, tail_values = (tails[:, : KV * DH], tails[:, KV * DH :])
    keys_ext = jnp.concatenate([tail_keys, key_b], axis=0)
    values_ext = jnp.concatenate([tail_values, value_b], axis=0)
    doc_pad = jnp.concatenate([jnp.full((band_len,), -1, jnp.int32), documents])
    doc_ext = lax.dynamic_slice_in_dim(doc_pad, first_row, band_len + local_rows)
    ext_places = first_row - band_len + jnp.arange(band_len + local_rows, dtype=jnp.int32)
    ext_places = ext_places[:, None]
    band_t = (doc_ext[:, None] == row_docs) & (ext_places <= row_places)
    band_t = (band_t & (ext_places > row_places - band_len)).astype(jnp.float32)
    banded_t, grad_qb_t, key_heads, value_heads = attend(
        band_t, query_b.T, keys_ext, values_ext, None, grad_out[0].T
    )
    banded, grad_qb = (banded_t.T, grad_qb_t.T)
    key_ext_grad, value_ext_grad = (from_heads(key_heads), from_heads(value_heads))
    heads = jnp.concatenate([key_ext_grad[:band_len], value_ext_grad[:band_len]], axis=1)
    heads = from_behind(heads.astype(jnp.bfloat16), "ctx", -1).astype(jnp.float32)
    head_keys, head_values = (heads[:, : KV * DH], heads[:, KV * DH :])
    grad_kb = key_ext_grad[band_len:].at[local_rows - band_len :].add(head_keys)
    grad_vb = value_ext_grad[band_len:].at[local_rows - band_len :].add(head_values)
    grad_kb = (grad_kb * DH ** (-0.5)).astype(jnp.bfloat16)
    grad_vb = grad_vb.astype(jnp.bfloat16)
    grad_proj = jnp.concatenate([grad_qb, grad_kb, grad_vb], axis=1)
    grad_normed = jnp.dot(grad_proj, w_b.T, preferred_element_type=jnp.float32)
    middle = jnp.mean(grad_normed * normed, axis=-1, keepdims=True)
    grad_mid = (
        grad_resid[0].astype(jnp.float32) + inverse_rms * (grad_normed - normed * middle)
    ).astype(jnp.bfloat16)
    grad_attended = jnp.dot(grad_mid, w_o.T, preferred_element_type=jnp.float32).astype(
        jnp.bfloat16
    )
    grad_query_t, key_heads, value_heads = attend(
        allowed_t, query_t, keys, values, attended_t, grad_attended.T
    )
    grad_query = grad_query_t.T
    key_sums, value_sums = (from_heads(key_heads), from_heads(value_heads))
    if own_kernels:
        norm_t = normed_bf.T.reshape(fsdp_count, -1, local_rows)
        kv_sums = jnp.concatenate([key_sums, value_sums], axis=1).astype(jnp.bfloat16)
        out_share, qkv_share, own_kv = reduce_weights(
            attended_t, norm_t, grad_mid, grad_proj, kv_sums
        )
        own_keys, own_values = (own_kv[:, : KV * DH], own_kv[:, KV * DH :])
        grad_w_out, grad_w_qkv = (out_share.astype(jnp.float32), qkv_share.astype(jnp.float32))
    else:
        own_keys, own_values = (
            lax.psum_scatter(
                key_sums.astype(jnp.bfloat16), "ctx", scatter_dimension=0, tiled=True
            ).astype(jnp.float32),
            lax.psum_scatter(
                value_sums.astype(jnp.bfloat16), "ctx", scatter_dimension=0, tiled=True
            ).astype(jnp.float32),
        )
        piece = normed_bf
        qkv_share = lax.psum_scatter(
            jnp.einsum("tf,tc->fc", piece, grad_proj, preferred_element_type=jnp.float32).astype(
                jnp.bfloat16
            ),
            "fsdp",
            scatter_dimension=0,
            tiled=True,
        )
        piece = attended
        out_share = lax.psum_scatter(
            jnp.einsum("tf,tc->fc", piece, grad_mid, preferred_element_type=jnp.float32).astype(
                jnp.bfloat16
            ),
            "fsdp",
            scatter_dimension=0,
            tiled=True,
        )
        grad_w_out, grad_w_qkv = (
            lax.psum(out_share, "ctx").astype(jnp.float32),
            lax.psum(qkv_share, "ctx").astype(jnp.float32),
        )
    grad_key = (own_keys * DH ** (-0.5)).astype(jnp.bfloat16)
    grad_value = own_values.astype(jnp.bfloat16)
    return (
        banded[None],
        grad_mid[None],
        grad_query[None],
        grad_key[None],
        grad_value[None],
        grad_w_out,
        grad_w_qkv,
    )


def solution(mesh):
    in_specs = (
        P("fsdp", "ctx", None),
        P("fsdp", "ctx", None),
        P("fsdp", "ctx", None),
        P("fsdp", "ctx", None),
        P("fsdp", None),
        P("fsdp", None),
        P("fsdp", None),
        P("fsdp", "ctx", None),
        P("fsdp", "ctx", None),
    )
    out_specs = (
        P("fsdp", "ctx", None),
        P("fsdp", "ctx", None),
        P("fsdp", "ctx", None),
        P("fsdp", "ctx", None),
        P("fsdp", "ctx", None),
        P("fsdp", None),
        P("fsdp", None),
    )
    return jax.shard_map(
        per_device, mesh=mesh, in_specs=in_specs, out_specs=out_specs, check_vma=False
    )
```
